32 devices in a mesh: island: 4 (over y, core), shard: 8 (over z, x).
Axes of the slice: x: 2, y: 2, z: 4, core: 2. Of those that a mesh axis runs over, the one named last changes fastest.
Arguments:
- pseudo_grad: float32 [4, 2048, 4096], P('island', 'shard'), may hold values from -6 to 6
- error_buffer: float32 [4, 2048, 4096], P('island', 'shard'), may hold values from -6 to 6
- momentum: float32 [2048, 4096], P('shard'), may hold values from -4 to 4
- weights: bfloat16 [2048, 4096], P('shard'), may hold values from -6 to 6
- warm_basis: float32 [2048, 64], P('shard'), may hold values from -6 to 6
Outputs:
- new_error: float32 [4, 2048, 4096], P('island', 'shard')
- new_momentum: float32 [2048, 4096], P('shard')
- new_weights: bfloat16 [2048, 4096], P('shard')
- new_basis: float32 [2048, 64], P('shard')
The draws below stay inside these ranges and needn't reach their ends.
All inputs are finite; a program needn't handle non-finite values.
Results may differ from the reference program's by a relative error of at most 0.001.
Values sent between devices are 32-bit elements; how exact they have to be, the bound alone decides.
A program may use at most 128 MiB of HBM per device.

```python
import jax
import jax.numpy as jnp
from jax import lax

D = 4096
RANK = 64
ITERS = 2
FF = 2048
N_ISLAND = 4


def level_of(key, dims, pieces, least, largest):
    factor_of = 1.0
    for position, shards_of in pieces:
        draws = jax.random.uniform(jax.random.fold_in(jax.random.fold_in(key, 6), position), (shards_of,), jnp.float32, least / len(pieces), largest / len(pieces))
        factor_of = factor_of * jnp.repeat(jnp.exp(draws), dims[position] // shards_of).reshape((-1,) + (1,) * (len(dims) - 1 - position))
    return factor_of


def bell_draw(rng, dims, deviation, limit, split=(), kind=jnp.bfloat16):
    level = level_of(rng, dims, split, -0.22, 0.18) if split else 1.0
    array = jax.random.normal(rng, dims, jnp.float32) * deviation * level
    return jnp.minimum(jnp.maximum(array, -limit), limit).astype(kind)


def setup_inputs(seed: int = 0) -> dict:
    arg_keys = jax.random.split(jax.random.key(seed), 6)
    return {
        "pseudo_grad": bell_draw(arg_keys[0], (N_ISLAND, FF, D), 1.0, 6.0, ((0, 4), (1, 8)), jnp.float32),
        "error_buffer": bell_draw(arg_keys[1], (N_ISLAND, FF, D), 0.5, 6.0, ((0, 4), (1, 8)), jnp.float32),
        "momentum": bell_draw(arg_keys[2], (FF, D), 0.3, 4.0, ((0, 8),), jnp.float32),
        "weights": bell_draw(arg_keys[3], (FF, D), 1.0, 6.0, ((0, 8),)),
        "warm_basis": bell_draw(arg_keys[4], (FF, RANK), 1.0, 6.0, ((0, 8),), jnp.float32),
    }


HIGH = lax.Precision.HIGHEST
outer_beta = 0.9
outer_rate = 0.7

def orthonormal(factor_rows):
    gram_matrix = jnp.dot(factor_rows, factor_rows.T, precision=HIGH)
    lower_factor = jnp.linalg.cholesky(gram_matrix)
    return lax.linalg.triangular_solve(lower_factor, factor_rows, left_side=True, lower=True)

def reference(pseudo_grad, error_buffer, momentum, weights, warm_basis):
    merged = pseudo_grad + error_buffer
    summed = jnp.sum(merged, axis=0)
    basis_now = warm_basis
    for iteration in range(ITERS):
        factor_rows = orthonormal(jnp.dot(basis_now.T, summed, precision=HIGH))
        local_proj = jnp.einsum('ifd,rd->ifr', merged, factor_rows, precision=HIGH)
        basis_now = jnp.sum(local_proj, axis=0)
    new_error = merged - jnp.einsum('ifr,rd->ifd', local_proj, factor_rows, precision=HIGH)
    update = jnp.dot(basis_now / N_ISLAND, factor_rows, precision=HIGH)
    new_momentum = outer_beta * momentum + update
    stepped = weights.astype(jnp.float32) - outer_rate * (update + outer_beta * new_momentum)
    return (new_error, new_momentum, stepped.astype(jnp.bfloat16), basis_now)
```

```python
import functools

import jax
import jax.numpy as jnp
from jax import lax
from jax.experimental import pallas as pl
from jax.experimental.pallas import tpu as pltpu
from jax.sharding import PartitionSpec as P

ITERS = 2

HIGH = lax.Precision.HIGH
HIGHEST = lax.Precision.HIGHEST
outer_beta = 0.9
outer_rate = 0.7
MESH = pl.DeviceIdType.MESH
LANES = 128


def wait_bytes(ref, sem):
    pltpu.make_async_copy(ref, ref, sem).wait()


def reduce_all_kernel(
    n_island, n_shard, p_ref, out_ref, pair_buf, half, terms, pair_send, pair_recv, rs_send, rs_recv, ag_send, ag_recv, fw_send, fw_recv
):
    island, shard = lax.axis_index("island"), lax.axis_index("shard")
    core, row = lax.rem(island, 2), island // 2
    peers = (n_island // 2) * n_shard
    me = row * n_shard + shard
    width = half.shape[1]
    _, rows, cols = terms.shape
    groups = half.shape[0] // rows
    partner = (island + 1 - 2 * core, shard)

    def device(k):
        return ((k // n_shard) * 2 + core, lax.rem(k, n_shard))

    def chunk(ref, k, base):
        start = pl.multiple_of(base + (k // groups) * cols, LANES)
        if groups == 1:
            return ref.at[:, pl.ds(start, cols)]
        return ref.at[pl.ds(pl.multiple_of(lax.rem(k, groups) * rows, 8), rows), pl.ds(start, cols)]

    def each_peer(body):
        @pl.loop(1, peers)
        def _(d):
            body(lax.rem(me + d, peers))

    mine = pl.multiple_of(core * width, LANES)
    other = pl.multiple_of((1 - core) * width, LANES)

    barrier = pltpu.get_barrier_semaphore()
    pl.semaphore_signal(barrier, inc=1, device_id=partner, device_id_type=MESH)
    each_peer(lambda k: pl.semaphore_signal(barrier, inc=1, device_id=device(k), device_id_type=MESH))
    pl.semaphore_wait(barrier, peers)

    pair = pltpu.make_async_remote_copy(
        src_ref=p_ref.at[:, pl.ds(other, width)], dst_ref=pair_buf, send_sem=pair_send, recv_sem=pair_recv, device_id=partner, device_id_type=MESH
    )
    pair.start()
    pair.wait()
    half[...] = p_ref[:, pl.ds(mine, width)] + pair_buf[...]

    def send_term(k):
        pltpu.make_async_remote_copy(
            src_ref=chunk(half, k, 0), dst_ref=terms.at[me], send_sem=rs_send, recv_sem=rs_recv, device_id=device(k), device_id_type=MESH
        ).start()

    each_peer(send_term)
    total = chunk(half, me, 0)[...]
    some = terms.at[pl.ds(0, peers - 1)]
    wait_bytes(some, rs_recv)
    total = lax.fori_loop(1, peers, lambda d, t: t + terms[lax.rem(me + d, peers)], total)
    chunk(out_ref, me, mine)[...] = total
    wait_bytes(some, rs_send)

    def copy_out(k, target, send, recv):
        return pltpu.make_async_remote_copy(
            src_ref=chunk(out_ref, k, mine), dst_ref=chunk(out_ref, k, mine), send_sem=send, recv_sem=recv, device_id=target, device_id_type=MESH
        )

    each_peer(lambda k: copy_out(me, device(k), ag_send, ag_recv.at[me]).start())
    copy_out(me, partner, fw_send, fw_recv).start()

    def forward(k):
        copy_out(k, partner, ag_send, ag_recv.at[k]).wait_recv()
        copy_out(k, partner, fw_send, fw_recv).start()

    each_peer(forward)
    wait_bytes(some, ag_send)
    wait_bytes(half, fw_send)
    wait_bytes(half, fw_recv)


def reduce_all(p, n_island, n_shard, ident):
    rank, dim = p.shape
    peers = (n_island // 2) * n_shard
    width = dim // 2
    groups = max(1, peers * LANES // width)
    rows, cols = rank // groups, width * groups // peers
    f32 = jnp.float32
    sem = pltpu.SemaphoreType.DMA
    return pl.pallas_call(
        functools.partial(reduce_all_kernel, n_island, n_shard),
        out_shape=jax.ShapeDtypeStruct((rank, dim), f32),
        in_specs=[pl.BlockSpec(memory_space=pltpu.VMEM)],
        out_specs=pl.BlockSpec(memory_space=pltpu.VMEM),
        scratch_shapes=[
            pltpu.VMEM((rank, width), f32),
            pltpu.VMEM((rank, width), f32),
            pltpu.VMEM((peers, rows, cols), f32),
            sem, sem, sem, sem, sem, sem((peers,)), sem, sem,
        ],
        compiler_params=pltpu.CompilerParams(collective_id=ident, has_side_effects=True),
        name="reduce_all",
    )(p)


def island_kernel(n_island, x_ref, out_ref, terms, send_sem, recv_sem):
    island, shard = lax.axis_index("island"), lax.axis_index("shard")
    peers = [lax.rem(island + d, n_island) for d in range(1, n_island)]
    barrier = pltpu.get_barrier_semaphore()
    for k in peers:
        pl.semaphore_signal(barrier, inc=1, device_id=(k, shard), device_id_type=MESH)
    pl.semaphore_wait(barrier, n_island - 1)
    copies = [
        pltpu.make_async_remote_copy(
            src_ref=x_ref, dst_ref=terms.at[d], send_sem=send_sem.at[d], recv_sem=recv_sem.at[d], device_id=(k, shard), device_id_type=MESH
        )
        for d, k in enumerate(peers)
    ]
    for copy in copies:
        copy.start()
    total = x_ref[...]
    for copy in copies:
        copy.wait()
    total = None
    for i in range(n_island):
        slot = lax.rem(island - i + n_island, n_island)
        term = jnp.where(slot == 0, x_ref[...], terms[jnp.maximum(slot - 1, 0)])
        total = term if total is None else total + term
    out_ref[...] = total


def reduce_island(x, n_island, ident):
    sem = pltpu.SemaphoreType.DMA
    return pl.pallas_call(
        functools.partial(island_kernel, n_island),
        out_shape=jax.ShapeDtypeStruct(x.shape, jnp.float32),
        in_specs=[pl.BlockSpec(memory_space=pltpu.VMEM)],
        out_specs=pl.BlockSpec(memory_space=pltpu.VMEM),
        scratch_shapes=[pltpu.VMEM((n_island - 1,) + x.shape, jnp.float32), sem((n_island - 1,)), sem((n_island - 1,))],
        compiler_params=pltpu.CompilerParams(collective_id=ident, has_side_effects=True),
        name="reduce_island",
    )(x)


def orthonormal(factor_rows):
    gram_matrix = jnp.dot(factor_rows, factor_rows.T, precision=HIGHEST)
    lower_factor = jnp.linalg.cholesky(gram_matrix)
    return lax.linalg.triangular_solve(lower_factor, factor_rows, left_side=True, lower=True)


def on_device(n_island, n_shard, pseudo_grad, error_buffer, momentum, weights, warm_basis):
    merged = (pseudo_grad + error_buffer)[0]
    basis_rows = warm_basis.T
    for iteration in range(ITERS):
        partial_value = jnp.dot(basis_rows, merged, precision=HIGH)
        factor_rows = orthonormal(reduce_all(partial_value, n_island, n_shard, 0))
        local_rows = lax.dot_general(factor_rows, merged, (((1,), (1,)), ((), ())), precision=HIGH)
        basis_rows = reduce_island(local_rows, n_island, 1)
    new_error = merged - jnp.dot(local_rows.T, factor_rows, precision=HIGH)
    update = jnp.dot(basis_rows.T / n_island, factor_rows, precision=HIGH)
    new_momentum = outer_beta * momentum + update
    stepped = weights.astype(jnp.float32) - outer_rate * (update + outer_beta * new_momentum)
    return (new_error[None], new_momentum, stepped.astype(jnp.bfloat16), basis_rows.T)


def solution(mesh):
    in_specs = (
        P("island", "shard", None),
        P("island", "shard", None),
        P("shard", None),
        P("shard", None),
        P("shard", None),
    )
    out_specs = (P("island", "shard", None), P("shard", None), P("shard", None), P("shard", None))
    body = functools.partial(on_device, mesh.shape["island"], mesh.shape["shard"])
    return jax.shard_map(body, mesh=mesh, in_specs=in_specs, out_specs=out_specs, check_vma=False)
```

```python
import functools

import jax
import jax.numpy as jnp
from jax import lax
from jax.experimental import pallas as pl
from jax.experimental.pallas import tpu as pltpu
from jax.sharding import PartitionSpec as P

ITERS = 2

HIGH = lax.Precision.HIGH
HIGHEST = lax.Precision.HIGHEST
outer_beta = 0.9
outer_rate = 0.7
MESH = pl.DeviceIdType.MESH
LANES = 128


def wait_bytes(ref, sem):
    pltpu.make_async_copy(ref, ref, sem).wait()


def reduce_all_kernel(
    n_island, n_shard, p_ref, out_ref, pair_buf, half, terms, pair_send, pair_recv, rs_send, rs_recv, ag_send, ag_recv, fw_send, fw_recv
):
    island, shard = lax.axis_index("island"), lax.axis_index("shard")
    core, row = lax.rem(island, 2), island // 2
    peers = (n_island // 2) * n_shard
    me = row * n_shard + shard
    width = half.shape[1]
    _, rows, cols = terms.shape
    groups = half.shape[0] // rows
    partner = (island + 1 - 2 * core, shard)

    def device(k):
        return ((k // n_shard) * 2 + core, lax.rem(k, n_shard))

    def chunk(ref, k, base):
        start = pl.multiple_of(base + (k // groups) * cols, LANES)
        if groups == 1:
            return ref.at[:, pl.ds(start, cols)]
        return ref.at[pl.ds(pl.multiple_of(lax.rem(k, groups) * rows, 8), rows), pl.ds(start, cols)]

    def each_peer(body):
        @pl.loop(1, peers)
        def _(d):
            body(lax.rem(me + d, peers))

    mine = pl.multiple_of(core * width, LANES)
    other = pl.multiple_of((1 - core) * width, LANES)

    barrier = pltpu.get_barrier_semaphore()
    pl.semaphore_signal(barrier, inc=1, device_id=partner, device_id_type=MESH)
    each_peer(lambda k: pl.semaphore_signal(barrier, inc=1, device_id=device(k), device_id_type=MESH))
    pl.semaphore_wait(barrier, peers)

    pair = pltpu.make_async_remote_copy(
        src_ref=p_ref.at[:, pl.ds(other, width)], dst_ref=pair_buf, send_sem=pair_send, recv_sem=pair_recv, device_id=partner, device_id_type=MESH
    )
    pair.start()
    pair.wait()
    half[...] = p_ref[:, pl.ds(mine, width)] + pair_buf[...]

    def send_term(k):
        pltpu.make_async_remote_copy(
            src_ref=chunk(half, k, 0), dst_ref=terms.at[me], send_sem=rs_send, recv_sem=rs_recv, device_id=device(k), device_id_type=MESH
        ).start()

    each_peer(send_term)
    total = chunk(half, me, 0)[...]
    some = terms.at[pl.ds(0, peers - 1)]
    wait_bytes(some, rs_recv)
    total = lax.fori_loop(1, peers, lambda d, t: t + terms[lax.rem(me + d, peers)], total)
    chunk(out_ref, me, mine)[...] = total
    wait_bytes(some, rs_send)

    def copy_out(k, target, send, recv):
        return pltpu.make_async_remote_copy(
            src_ref=chunk(out_ref, k, mine), dst_ref=chunk(out_ref, k, mine), send_sem=send, recv_sem=recv, device_id=target, device_id_type=MESH
        )

    each_peer(lambda k: copy_out(me, device(k), ag_send, ag_recv.at[me]).start())
    copy_out(me, partner, fw_send, fw_recv).start()

    def forward(k):
        copy_out(k, partner, ag_send, ag_recv.at[k]).wait_recv()
        copy_out(k, partner, fw_send, fw_recv).start()

    each_peer(forward)
    wait_bytes(some, ag_send)
    wait_bytes(half, fw_send)
    wait_bytes(half, fw_recv)


def reduce_all(p, n_island, n_shard, ident):
    rank, dim = p.shape
    peers = (n_island // 2) * n_shard
    width = dim // 2
    groups = max(1, peers * LANES // width)
    rows, cols = rank // groups, width * groups // peers
    f32 = jnp.float32
    sem = pltpu.SemaphoreType.DMA
    return pl.pallas_call(
        functools.partial(reduce_all_kernel, n_island, n_shard),
        out_shape=jax.ShapeDtypeStruct((rank, dim), f32),
        in_specs=[pl.BlockSpec(memory_space=pltpu.VMEM)],
        out_specs=pl.BlockSpec(memory_space=pltpu.VMEM),
        scratch_shapes=[
            pltpu.VMEM((rank, width), f32),
            pltpu.VMEM((rank, width), f32),
            pltpu.VMEM((peers, rows, cols), f32),
            sem, sem, sem, sem, sem, sem((peers,)), sem, sem,
        ],
        compiler_params=pltpu.CompilerParams(collective_id=ident, has_side_effects=True),
        name="reduce_all",
    )(p)


def island_kernel(n_island, x_ref, out_ref, terms, send_sem, recv_sem):
    island, shard = lax.axis_index("island"), lax.axis_index("shard")
    peers = [lax.rem(island + d, n_island) for d in range(1, n_island)]
    barrier = pltpu.get_barrier_semaphore()
    for k in peers:
        pl.semaphore_signal(barrier, inc=1, device_id=(k, shard), device_id_type=MESH)
    pl.semaphore_wait(barrier, n_island - 1)
    copies = [
        pltpu.make_async_remote_copy(
            src_ref=x_ref, dst_ref=terms.at[d], send_sem=send_sem.at[d], recv_sem=recv_sem.at[d], device_id=(k, shard), device_id_type=MESH
        )
        for d, k in enumerate(peers)
    ]
    for copy in copies:
        copy.start()
    total = x_ref[...]
    for copy in copies:
        copy.wait()
    total = None
    for i in range(n_island):
        slot = lax.rem(island - i + n_island, n_island)
        term = jnp.where(slot == 0, x_ref[...], terms[jnp.maximum(slot - 1, 0)])
        total = term if total is None else total + term
    out_ref[...] = total


def reduce_island(x, n_island, ident):
    sem = pltpu.SemaphoreType.DMA
    return pl.pallas_call(
        functools.partial(island_kernel, n_island),
        out_shape=jax.ShapeDtypeStruct(x.shape, jnp.float32),
        in_specs=[pl.BlockSpec(memory_space=pltpu.VMEM)],
        out_specs=pl.BlockSpec(memory_space=pltpu.VMEM),
        scratch_shapes=[pltpu.VMEM((n_island - 1,) + x.shape, jnp.float32), sem((n_island - 1,)), sem((n_island - 1,))],
        compiler_params=pltpu.CompilerParams(collective_id=ident, has_side_effects=True),
        name="reduce_island",
    )(x)


def orthonormal_kernel(p_ref, out_ref):
    p = p_ref[...]
    rank = p.shape[0]
    gram = lax.dot_general(p, p, (((1,), (1,)), ((), ())), precision=HIGHEST, preferred_element_type=jnp.float32)
    step = 8
    tiles = rank // step
    left = [gram[t * step : (t + 1) * step] for t in range(tiles)]
    row_id = lax.broadcasted_iota(jnp.int32, (step, rank), 0)
    col_id = lax.broadcasted_iota(jnp.int32, (step, rank), 1)
    diagonal = [row_id + t * step == col_id for t in range(tiles)]
    right = [jnp.where(d, 1.0, 0.0) for d in diagonal]
    for j in range(rank):
        t, s = divmod(j, step)
        row, side = left[t][s : s + 1], right[t][s : s + 1]
        row_over = row / left[t][s : s + 1, j : j + 1]
        side_over = side / left[t][s : s + 1, j : j + 1]
        for u in range(t, tiles):
            col = left[u][:, j : j + 1]
            if u == t:
                col = jnp.where(row_id[:, :1] > s, col, 0.0)
            left[u] = left[u] - col * row_over
            right[u] = right[u] - col * side_over
    for t in range(tiles):
        pivot = jnp.sum(jnp.where(diagonal[t], left[t], 0.0), axis=1, keepdims=True)
        right[t] = right[t] / jnp.sqrt(pivot)
    inverse = jnp.concatenate(right, axis=0)
    out_ref[...] = jnp.dot(inverse, p, precision=HIGHEST, preferred_element_type=jnp.float32)


def orthonormal(factor_rows):
    return pl.pallas_call(
        orthonormal_kernel,
        out_shape=jax.ShapeDtypeStruct(factor_rows.shape, jnp.float32),
        in_specs=[pl.BlockSpec(memory_space=pltpu.VMEM)],
        out_specs=pl.BlockSpec(memory_space=pltpu.VMEM),
        name="orthonormal",
    )(factor_rows)


def on_device(n_island, n_shard, pseudo_grad, error_buffer, momentum, weights, warm_basis):
    merged = (pseudo_grad + error_buffer)[0]
    basis_rows = warm_basis.T
    for iteration in range(ITERS):
        partial_value = jnp.dot(basis_rows, merged, precision=HIGH)
        factor_rows = orthonormal(reduce_all(partial_value, n_island, n_shard, 0))
        local_rows = lax.dot_general(factor_rows, merged, (((1,), (1,)), ((), ())), precision=HIGH)
        basis_rows = reduce_island(local_rows, n_island, 1)
    new_error = merged - jnp.dot(local_rows.T, factor_rows, precision=HIGH)
    update = jnp.dot(basis_rows.T / n_island, factor_rows, precision=HIGH)
    new_momentum = outer_beta * momentum + update
    stepped = weights.astype(jnp.float32) - outer_rate * (update + outer_beta * new_momentum)
    return (new_error[None], new_momentum, stepped.astype(jnp.bfloat16), basis_rows.T)


def solution(mesh):
    in_specs = (
        P("island", "shard", None),
        P("island", "shard", None),
        P("shard", None),
        P("shard", None),
        P("shard", None),
    )
    out_specs = (P("island", "shard", None), P("shard", None), P("shard", None), P("shard", None))
    body = functools.partial(on_device, mesh.shape["island"], mesh.shape["shard"])
    return jax.shard_map(body, mesh=mesh, in_specs=in_specs, out_specs=out_specs, check_vma=False)
```
